16 devices in a mesh: tp: 2 (over z), dp: 8 (over y, x, core).
Axes of the slice: x: 2, y: 2, z: 2, core: 2. Of those that a mesh axis runs over, the one named last changes fastest.
Arguments:
- hidden: bfloat16 [8, 2048, 2048], P('dp')
- targets: int32 [8, 2048], P('dp')
- loss_mask: int32 [8, 2048], P('dp')
- norm_gain: float32 [2048], replicated
- head_w: bfloat16 [2048, 32256], P(None, 'tp')
Outputs:
- output 1: float32 [], replicated
- output 2: bfloat16 [8, 2048, 2048], P('dp')
- output 3: float32 [2048, 32256], P(None, 'tp')
- output 4: float32 [2048], replicated
All inputs are finite; a program needn't handle non-finite values.
Results may differ from the reference program's by a relative error of at most 0.001.
Values sent between devices are 32-bit elements.
A program may use at most 1 GiB of HBM per device.

```python
import jax
import jax.numpy as jnp
from jax import lax

BATCH_SIZE = 8
SEQ_LEN = 2048
HIDDEN_DIM = 2048
VOCAB_SIZE = 32256
DATA_SHARDS = 8
NORM_EPS = 1e-6


def setup_inputs(seed: int = 0) -> dict:
    rng_key = jax.random.key(seed)
    k_noise, k_head, k_gain, k_tgt, k_len, k_jit = jax.random.split(rng_key, 6)
    head_f = jax.random.normal(k_head, (HIDDEN_DIM, VOCAB_SIZE), jnp.float32) * HIDDEN_DIM ** -0.5
    targets = jax.random.randint(k_tgt, (BATCH_SIZE, SEQ_LEN), 0, VOCAB_SIZE, jnp.int32)
    targets = targets.at[0, 0].set(0).at[BATCH_SIZE - 1, SEQ_LEN - 1].set(VOCAB_SIZE - 1)
    rows_dev = BATCH_SIZE // DATA_SHARDS
    shard_len = jax.random.randint(k_len, (DATA_SHARDS, 1), SEQ_LEN // 2 + SEQ_LEN // 16, SEQ_LEN + 1, jnp.int32)
    jitter = jax.random.randint(k_jit, (DATA_SHARDS, rows_dev), 0, SEQ_LEN // 16 + 1, jnp.int32)
    seq_lens = (shard_len - jitter).reshape(BATCH_SIZE)
    loss_mask = (jnp.arange(SEQ_LEN)[None, :] < seq_lens[:, None]).astype(jnp.int32)
    tgt_cols = jnp.moveaxis(jnp.take(head_f, targets, axis=1), 0, -1)
    base_noise = jax.random.normal(k_noise, (BATCH_SIZE, SEQ_LEN, HIDDEN_DIM), jnp.float32)
    hidden = (base_noise + 5.0 * tgt_cols).astype(jnp.bfloat16)
    norm_gain = 2.5 + 0.75 * jax.random.normal(k_gain, (HIDDEN_DIM,), jnp.float32)
    return {'hidden': hidden, 'targets': targets, 'loss_mask': loss_mask, 'norm_gain': norm_gain, 'head_w': head_f.astype(jnp.bfloat16)}


def norm_forward(x_rows, norm_gain):
    x_float = x_rows.astype(jnp.float32)
    inv_rms = lax.rsqrt(jnp.mean(x_float * x_float, axis=-1, keepdims=True) + NORM_EPS)
    normed = x_float * inv_rms
    return normed, inv_rms, (normed * norm_gain).astype(jnp.bfloat16)


def reference(hidden, targets, loss_mask, norm_gain, head_w):
    n_blocks = BATCH_SIZE * SEQ_LEN // 128
    x_blocks = hidden.reshape(n_blocks, 128, HIDDEN_DIM)
    tgt_blocks = targets.reshape(n_blocks, 128, 1)
    weight_blocks = loss_mask.reshape(n_blocks, 128, 1).astype(jnp.float32)
    tok_count = jnp.sum(weight_blocks)
    vocab_ids = jnp.arange(VOCAB_SIZE)[None, :]

    def scan_step(acc_state, blk_in):
        head_acc, gain_acc, loss_acc = acc_state
        x_rows, tgt_ids, tok_weight = blk_in
        normed, inv_rms, u_rows = norm_forward(x_rows, norm_gain)
        logits = jnp.dot(u_rows, head_w, preferred_element_type=jnp.float32)
        row_max = jnp.max(logits, axis=-1, keepdims=True)
        shifted = jnp.exp(logits - row_max)
        exp_sum = jnp.sum(shifted, axis=-1, keepdims=True)
        log_norm = row_max + jnp.log(exp_sum)
        is_target = vocab_ids == tgt_ids
        tgt_logit = jnp.sum(jnp.where(is_target, logits, 0.0), axis=-1, keepdims=True)
        loss_acc = loss_acc + jnp.sum(tok_weight * (log_norm - tgt_logit))
        grad_logits = ((shifted / exp_sum - is_target.astype(jnp.float32)) * (tok_weight / tok_count)).astype(jnp.bfloat16)
        grad_u = jnp.dot(grad_logits, head_w.T, preferred_element_type=jnp.float32)
        head_acc = head_acc + jnp.dot(u_rows.T, grad_logits, preferred_element_type=jnp.float32)
        grad_normed = grad_u * norm_gain
        grad_rows = inv_rms * (grad_normed - normed * jnp.mean(grad_normed * normed, axis=-1, keepdims=True))
        gain_acc = gain_acc + jnp.sum(grad_u * normed, axis=0)
        return (head_acc, gain_acc, loss_acc), grad_rows.astype(jnp.bfloat16)

    init_state = (jnp.zeros((HIDDEN_DIM, VOCAB_SIZE), jnp.float32), jnp.zeros((HIDDEN_DIM,), jnp.float32), jnp.zeros((), jnp.float32))
    final_state, grad_blocks = lax.scan(scan_step, init_state, (x_blocks, tgt_blocks, weight_blocks))
    grad_head, grad_gain, loss_acc = final_state
    return loss_acc / tok_count, grad_blocks.reshape(BATCH_SIZE, SEQ_LEN, HIDDEN_DIM), grad_head, grad_gain
```

```python
import functools

import jax
import jax.numpy as jnp
from jax import lax
from jax.experimental import pallas as pl
from jax.experimental.pallas import tpu as pltpu
from jax.sharding import PartitionSpec as P

NORM_EPS = 1e-6

X_PAIRS = [(d, d ^ 2) for d in range(8)]
Y_PAIRS = [(d, d ^ 4) for d in range(8)]
CORE_PAIRS = [(d, d ^ 1) for d in range(8)]
Z_PAIRS = [(0, 1), (1, 0)]

TILE = 128
CHUNKS = (4, 4, 4, 3)
REST = {8: 4, 9: 2}
ROW_BLOCK = 1024


def norm_forward(x_float, norm_gain):
    inv_rms = lax.rsqrt(jnp.mean(x_float * x_float, axis=-1, keepdims=True) + NORM_EPS)
    normed = x_float * inv_rms
    return normed, inv_rms, (normed * norm_gain).astype(jnp.bfloat16)


def norm_backward(grad_u, normed, inv_rms, norm_gain):
    grad_normed = grad_u * norm_gain
    grad_rows = inv_rms * (grad_normed - normed * jnp.mean(grad_normed * normed, axis=-1, keepdims=True))
    return grad_rows.astype(jnp.bfloat16), jnp.sum(grad_u * normed, axis=0)


def to_x(v):
    return lax.ppermute(v, 'dp', X_PAIRS)


def to_y(v):
    return lax.ppermute(v, 'dp', Y_PAIRS)


def to_core(v):
    return lax.ppermute(v, 'dp', CORE_PAIRS)


def to_z(v):
    return lax.ppermute(v, 'tp', Z_PAIRS)


def sync(*values):
    return lax.optimization_barrier(values)


def uninit(shape, dtype):
    return pl.pallas_call(lambda o_ref: None, out_shape=jax.ShapeDtypeStruct(shape, dtype), out_specs=pl.BlockSpec(memory_space=pl.ANY))()


def head_kernel(width, rows_of, n_steps, idx_ref, *refs):
    n = len(rows_of)
    if width:
        (u_ref, w_ref, lse_ref, scale_ref, tgt_ref), refs = refs[:5], refs[5:]
    pieces, refs = refs[:n], refs[n + 1:]
    if width:
        out_ref, refs = refs[0], refs[1:]
    whole_ref, refs = refs[0], refs[1:]
    bufs, in_sem, out_sem = refs[:n], refs[n], refs[n + 1]
    i = pl.program_id(0)

    def load(p):
        return pltpu.make_async_copy(pieces[p], bufs[p], in_sem.at[p])

    def store(p):
        rows, cols = pieces[p].shape
        col = pl.multiple_of(idx_ref[1 + p] * TILE, TILE)
        return pltpu.make_async_copy(bufs[p], whole_ref.at[pl.ds(rows_of[p], rows), pl.ds(col, cols)], out_sem.at[p])

    if n:
        @pl.when(i == 0)
        def _():
            for p in range(n):
                load(p).start()

        @pl.when(i == min(2, n_steps - 1))
        def _():
            for p in range(n):
                load(p).wait()
                store(p).start()

    if width:
        @pl.when(i == 0)
        def _():
            out_ref[...] = jnp.zeros_like(out_ref)

        u = u_ref[...]
        z = jnp.dot(u, w_ref[...], preferred_element_type=jnp.float32)
        hit = (lax.broadcasted_iota(jnp.int32, z.shape, 1) + idx_ref[0] * width) == tgt_ref[...]
        dz = ((jnp.exp(z - lse_ref[...]) - jnp.where(hit, 1.0, 0.0)) * scale_ref[...]).astype(jnp.bfloat16)
        out_ref[...] += lax.dot_general(u, dz, (((0,), (0,)), ((), ())), preferred_element_type=jnp.float32)

    if n:
        @pl.when(i == n_steps - 1)
        def _():
            for p in range(n):
                store(p).wait()


def head_part(operands, blk, width, pieces, whole):
    u, head_w, lse, scale, tgt = operands
    rows, hid = u.shape
    steps = rows // ROW_BLOCK if width else 1
    col = pl.BlockSpec((ROW_BLOCK, 1), lambda i, b: (i, 0))
    hbm = pl.BlockSpec(memory_space=pl.ANY)
    n = len(pieces)
    idx = jnp.stack([jnp.asarray(v, jnp.int32) for v in [blk] + [p[2] for p in pieces]])
    comp_in = [pl.BlockSpec((ROW_BLOCK, hid), lambda i, b: (i, 0)), pl.BlockSpec((hid, width), lambda i, b: (0, b[0])), col, col, col] if width else []
    comp_out = [pl.BlockSpec((hid, width), lambda i, b: (0, 0))] if width else []
    comp_shape = [jax.ShapeDtypeStruct((hid, width), jnp.float32)] if width else []
    res = pl.pallas_call(
        functools.partial(head_kernel, width, tuple(p[1] for p in pieces), steps),
        grid_spec=pltpu.PrefetchScalarGridSpec(
            num_scalar_prefetch=1,
            grid=(steps,),
            in_specs=comp_in + [hbm] * (n + 1),
            out_specs=comp_out + [hbm],
            scratch_shapes=[pltpu.VMEM(p[0].shape, jnp.float32) for p in pieces] + [pltpu.SemaphoreType.DMA((max(n, 1),))] * 2,
        ),
        out_shape=comp_shape + [jax.ShapeDtypeStruct(whole.shape, whole.dtype)],
        input_output_aliases={1 + len(comp_in) + n: len(comp_out)},
        compiler_params=pltpu.CompilerParams(vmem_limit_bytes=58 * 2**20, dimension_semantics=("arbitrary",)),
        cost_estimate=pl.CostEstimate(flops=4 * rows * hid * max(width, 32), bytes_accessed=2 * rows * hid, transcendentals=rows * width),
        name=f"head_{width}_{n}",
    )(idx, *([u, head_w, lse, scale, tgt] if width else []), *[p[0] for p in pieces], whole)
    return res if width else (None, res[0])


def forward_kernel(u_ref, w_ref, tgt_ref, z_ref, max_ref, sum_ref, hit_ref):
    i = pl.program_id(0)

    @pl.when(i == 0)
    def _():
        max_ref[...] = jnp.full_like(max_ref, jnp.finfo(jnp.float32).min)
        sum_ref[...] = jnp.zeros_like(sum_ref)
        hit_ref[...] = jnp.zeros_like(hit_ref)

    z = jnp.dot(u_ref[...], w_ref[...], preferred_element_type=jnp.float32)
    z_ref[...] = z
    groups = [z[:, k:k + TILE] for k in range(0, z.shape[1], TILE)]
    old = max_ref[...]
    new = functools.reduce(jnp.maximum, groups, old)
    max_ref[...] = new
    sum_ref[...] = sum_ref[...] * jnp.exp(old - new) + sum(jnp.exp(g - new) for g in groups)
    lane = tgt_ref[...] - lax.broadcasted_iota(jnp.int32, new.shape, 1) - i * z.shape[1]
    hit_ref[...] += sum(jnp.where(lane == k * TILE, g, 0.0) for k, g in enumerate(groups))


def forward_part(u, head_w, tgt):
    rows, hid = u.shape
    cols = head_w.shape[1]
    width = 6 * TILE
    stat = pl.BlockSpec((rows, TILE), lambda i: (0, 0))
    return pl.pallas_call(
        forward_kernel,
        grid=(cols // width,),
        in_specs=[pl.BlockSpec((rows, hid), lambda i: (0, 0)), pl.BlockSpec((hid, width), lambda i: (0, i)), pl.BlockSpec((rows, 1), lambda i: (0, 0))],
        out_specs=[pl.BlockSpec((rows, width), lambda i: (0, i)), stat, stat, stat],
        out_shape=[jax.ShapeDtypeStruct((rows, cols), jnp.float32)] + [jax.ShapeDtypeStruct((rows, TILE), jnp.float32)] * 3,
        compiler_params=pltpu.CompilerParams(vmem_limit_bytes=48 * 2**20, dimension_semantics=("arbitrary",)),
        cost_estimate=pl.CostEstimate(flops=2 * rows * hid * cols, bytes_accessed=4 * rows * cols, transcendentals=rows * cols),
        name="forward",
    )(u, head_w, tgt)


def rows_kernel(blk_ref, x_ref, gain_ref, mine_ref, other_ref, all_in_ref, out_ref, gain_out_ref):
    x = x_ref[...].astype(jnp.float32)
    inv_rms = lax.rsqrt(jnp.mean(x * x, axis=-1, keepdims=True) + NORM_EPS)
    normed = x * inv_rms
    grad_u = mine_ref[...] + other_ref[...]
    grad_normed = grad_u * gain_ref[...]
    out_ref[...] = (inv_rms * (grad_normed - normed * jnp.mean(grad_normed * normed, axis=-1, keepdims=True))).astype(jnp.bfloat16)
    gain_out_ref[...] = jnp.sum(grad_u * normed, axis=0, keepdims=True)


def rows_part(grad_rows, i, x_rows, gain, mine, other):
    n, hid = mine.shape
    one = pl.BlockSpec((1, hid), lambda k, b: (0, 0))
    blk = pl.BlockSpec((n, hid), lambda k, b: (b[0], 0))
    full = pl.BlockSpec((n, hid), lambda k, b: (0, 0))
    return pl.pallas_call(
        rows_kernel,
        grid_spec=pltpu.PrefetchScalarGridSpec(
            num_scalar_prefetch=1, grid=(1,),
            in_specs=[blk, one, full, full, pl.BlockSpec(memory_space=pl.ANY)],
            out_specs=[blk, one],
        ),
        out_shape=[jax.ShapeDtypeStruct(grad_rows.shape, grad_rows.dtype), jax.ShapeDtypeStruct((1, hid), jnp.float32)],
        input_output_aliases={5: 0},
        compiler_params=pltpu.CompilerParams(vmem_limit_bytes=32 * 2**20),
        cost_estimate=pl.CostEstimate(flops=1500 * n * hid, bytes_accessed=12 * n * hid, transcendentals=n),
        name="rows",
    )(jnp.full((1,), i, jnp.int32), x_rows, gain.reshape(1, hid), mine, other, grad_rows)


def put_kernel(blk_ref, x_ref, gain_ref, u_in_ref, u_ref):
    x = x_ref[...].astype(jnp.float32)
    inv_rms = lax.rsqrt(jnp.mean(x * x, axis=-1, keepdims=True) + NORM_EPS)
    u_ref[...] = (x * inv_rms * gain_ref[...]).astype(jnp.bfloat16)


def put_rows(u_all, rows, gain, start):
    n, hid = rows.shape
    return pl.pallas_call(
        put_kernel,
        grid_spec=pltpu.PrefetchScalarGridSpec(
            num_scalar_prefetch=1,
            grid=(n // 256,),
            in_specs=[pl.BlockSpec((256, hid), lambda i, b: (i, 0)), pl.BlockSpec((1, hid), lambda i, b: (0, 0)), pl.BlockSpec(memory_space=pl.ANY)],
            out_specs=pl.BlockSpec((256, hid), lambda i, b: (b[0] + i, 0)),
        ),
        out_shape=jax.ShapeDtypeStruct(u_all.shape, u_all.dtype),
        input_output_aliases={3: 0},
        compiler_params=pltpu.CompilerParams(vmem_limit_bytes=24 * 2**20),
        cost_estimate=pl.CostEstimate(flops=1500 * n * hid, bytes_accessed=6 * n * hid, transcendentals=n),
        name=f"put_{n}",
    )(jnp.asarray(start // 256, jnp.int32).reshape(1), rows, gain.reshape(1, hid), u_all)


def solution(mesh):
    def local_step(hidden, targets, loss_mask, norm_gain, head_w):
        n_rows, seq_len, hid = hidden.shape
        vocab_loc = head_w.shape[1]
        tokens = n_rows * seq_len
        tp = lax.axis_index('tp')
        dp = lax.axis_index('dp')
        chip, core = dp // 2, dp % 2
        vocab_off = tp * vocab_loc
        q = tokens // 4
        e = q // 2
        h = tokens // 2
        col_ids = jnp.arange(vocab_loc)[None, :]
        x_rows = hidden.reshape(tokens, hid)

        tm = lax.all_gather(jnp.stack([targets.reshape(tokens), loss_mask.reshape(tokens)]), 'dp')
        za, zo = tp * (tokens - q), (1 - tp) * (tokens - q)
        xa = lax.dynamic_slice(x_rows, (za, 0), (q, hid)).astype(jnp.float32)
        xa, tm, x_rows = sync(xa, tm, x_rows)
        w_all = tm[:, 1].astype(jnp.float32)
        tok_count = jnp.sum(w_all)
        scale_all = w_all / tok_count
        tgt_own = targets.reshape(tokens, 1) - vocab_off

        def block(c):
            return (chip ^ c) * tokens

        def put(u_all, rows, start):
            return put_rows(u_all, rows, norm_gain, start)

        def forward(i, u):
            s = slice(i * h, (i + 1) * h)
            logits, m, e_sum, hit = forward_part(u[s], head_w, tgt_own[s])
            loc_max = jnp.max(m, axis=-1, keepdims=True)
            return logits, loc_max[:, 0], jnp.sum(e_sum * jnp.exp(m - loc_max), axis=-1), jnp.sum(hit, axis=-1)

        rxa, rya = to_x(xa), to_y(xa)
        u_own = norm_forward(x_rows.astype(jnp.float32), norm_gain)[2]
        xb0, xb1 = x_rows[q:2 * q].astype(jnp.float32), x_rows[2 * q:3 * q].astype(jnp.float32)
        f0 = forward(0, u_own)
        rxa, rya, f0, u_own, xb0, xb1 = sync(rxa, rya, f0, u_own, xb0, xb1)
        rxb0, ryb0, oxa = to_x(xb0), to_y(xb0), to_z(rxa)
        f1 = forward(1, u_own)
        rxb0, ryb0, oxa, f1, rya, rxa, xb1, u_own = sync(rxb0, ryb0, oxa, f1, rya, rxa, xb1, u_own)
        stats = jnp.stack([jnp.concatenate([f[k] for f in (f0, f1)]) for k in (1, 2, 3)])
        fa, fb = rxa[:e], rya[e:]
        ga, gb = rxb0[:e], ryb0[e:]
        stats = lax.all_gather(stats, ('dp', 'tp'))
        stats, fa, fb, ga, gb, rya, xb1, u_own, rxa, rxb0, ryb0, oxa = sync(stats, fa, fb, ga, gb, rya, xb1, u_own, rxa, rxb0, ryb0, oxa)
        da1, da2, db01, db02 = to_y(fa), to_x(fb), to_y(ga), to_x(gb)
        oya = to_z(rya)
        stats = stats.reshape(8, 2, 3, tokens)
        row_max = jnp.max(stats[:, :, 0], axis=1)
        exp_sum = jnp.sum(stats[:, :, 1] * jnp.exp(stats[:, :, 0] - row_max[:, None]), axis=1)
        lse_all = row_max + jnp.log(exp_sum)
        tgt_logit = jnp.sum(stats[:, :, 2], axis=1)
        loss_mean = jnp.sum(w_all * (lse_all - tgt_logit)) / tok_count
        lse_own = lax.dynamic_index_in_dim(lse_all, dp, 0, False)[:, None]
        scale_own = lax.dynamic_index_in_dim(scale_all, dp, 0, False)[:, None]

        def backward(i, logits):
            s = slice(i * h, (i + 1) * h)
            hit = (col_ids == tgt_own[s]).astype(jnp.float32)
            dz = ((jnp.exp(logits - lse_own[s]) - hit) * scale_own[s]).astype(jnp.bfloat16)
            return lax.dot_general(dz, head_w, (((1,), (1,)), ((), ())), preferred_element_type=jnp.float32)

        u_all = uninit((4 * tokens, hid), jnp.bfloat16)
        g0 = backward(0, f0[0])
        u_all = put(u_all, rxa, block(1) + za)
        u_all = put(u_all, rya, block(2) + za)
        da1, da2, db01, db02, oya, g0, u_all, xb1, f1l, u_own, rxb0, ryb0, oxa = sync(da1, da2, db01, db02, oya, g0, u_all, xb1, f1[0], u_own, rxb0, ryb0, oxa)
        rxb1, ryb1, oda1, oda2 = to_x(xb1), to_y(xb1), to_z(da1), to_z(da2)
        g1 = backward(1, f1l)
        u_all = put(u_all, rxb0, block(1) + q)
        u_all = put(u_all, ryb0, block(2) + q)
        u_all = put(u_all, oxa, block(1) + zo)
        rxb1, ryb1, oda1, oda2, g1, u_all, ryb0, oxa, oya, da1, da2, db01, db02, u_own = sync(
            rxb1, ryb1, oda1, oda2, g1, u_all, ryb0, oxa, oya, da1, da2, db01, db02, u_own)
        db11, db12 = to_y(rxb1[:e]), to_x(ryb1[e:])
        for rows, start in ((oya, block(2) + zo), (da1, block(3) + za), (da2, block(3) + za + e),
                            (db01, block(3) + q), (db02, block(3) + q + e), (oda1, block(3) + zo), (oda2, block(3) + zo + e),
                            (rxb1, block(1) + 2 * q), (ryb1, block(2) + 2 * q)):
            u_all = put(u_all, rows, start)
        u_all = put(u_all, x_rows, block(0))

        def four(table):
            return lax.dynamic_index_in_dim(table.reshape(4, 2, tokens), core, 1, False).reshape(4 * tokens, 1)

        lse4, scale4, tgt4 = four(lse_all), four(scale_all), four(tm[:, 0]) - vocab_off
        grads = [g[i * 256:(i + 1) * 256] for g in (g0, g1) for i in range(h // 256)]
        db11, db12, u_all, grads, lse4, scale4, tgt4 = sync(db11, db12, u_all, grads, lse4, scale4, tgt4)
        u_all = put(u_all, db11, block(3) + 2 * q)
        u_all = put(u_all, db12, block(3) + 2 * q + e)

        firsts = [sum(CHUNKS[:j]) * 8 for j in range(len(CHUNKS))]
        half = hid // 2

        def at(j, c, k):
            return firsts[j] + ((chip ^ c) * 2 + k) * CHUNKS[j]

        out = uninit((hid, vocab_loc), jnp.float32)
        jobs = []
        for j in range(len(CHUNKS)):
            jobs += [('other', j), ('mine', j)]
        units = [(j, r) for j in range(len(CHUNKS)) for r in range(2)]
        hop1, hop2 = {}, {}
        gain_parts, gain_sum = [], None
        other = mine = rec = own_next = part = None
        ready = []
        grad_rows = uninit((tokens, hid), jnp.bfloat16)
        rest_at = sum(CHUNKS) * 8
        last = len(units) + 4
        for t in range(last + 1):
            job = jobs[t] if t < len(jobs) else None
            new = {}
            pieces, ready = ready, []
            share = []
            if 0 <= t - 2 < len(units):
                j, r = units[t - 2]
                if r == 0:
                    own_now = mine[:half] + rec[:half]
                    new['own'] = mine[half:] + rec[half:]
                else:
                    own_now = own_next
                own_now, = sync(own_now)
                new['hop1'] = (to_x(own_now), to_y(own_now))
                share.append((j, 0, r * half, own_now))
            if 0 <= t - 3 < len(units):
                j, r = units[t - 3]
                rx, ry = hop1[j, r]
                new['hop2'] = (to_y(rx[:half // 2]), to_x(ry[half // 2:]))
                share += [(j, 1, r * half, rx), (j, 2, r * half, ry)]
            if 0 <= t - 4 < len(units):
                j, r = units[t - 4]
                share += [(j, 3, r * half, hop2[j, r][0]), (j, 3, r * half + half // 2, hop2[j, r][1])]
            new['share'] = [to_core(v) for *_, v in share]
            if other is not None:
                new['rec'] = to_core(other)
            if t < len(grads):
                new['z'] = to_z(grads[t])
            if part is not None:
                new['rest_rec'], new['rest_own'] = to_core(part[0]), part[0]
                rest_tile = part[1]
            pieces = pieces + [(v, row, at(j, c, core)) for j, c, row, v in share]
            operands = (u_all, head_w, lse4, scale4, tgt4)
            if job:
                n = CHUNKS[job[1]]
                pos = chip * 2 + ((1 - core) if job[0] == 'other' else core)
                new[job[0]], out = head_part(operands, firsts[job[1]] // n + pos, n * TILE, pieces, out)
                pieces = []
            part = None
            if t in REST:
                n = REST[t]
                new['rest'], out = head_part(operands, rest_at // n, n * TILE, pieces, out)
                part = (None, rest_at)
                rest_at += n
            elif pieces and not job:
                _, out = head_part(operands, 0, 0, pieces, out)
            if 1 <= t <= len(grads):
                grad_rows, gain_part = rows_part(grad_rows, t - 1, x_rows, norm_gain, grads[t - 1], z_got)
                gain_parts.append(gain_part)
            if t > len(grads) and t - len(grads) <= 3:
                if t == len(grads) + 1:
                    gain_sum = sum(gain_parts)
                new['gain'] = (to_core, to_x, to_y)[t - len(grads) - 1](gain_sum)
            new, u_all, out, grads, x_rows, grad_rows, gain_parts, gain_sum = sync(new, u_all, out, grads, x_rows, grad_rows, gain_parts, gain_sum)
            other, own_next = new.get('other'), new.get('own')
            if part is not None:
                part = (new['rest'], part[1])
            if 'mine' in new:
                mine, rec = new['mine'], new['rec']
            if 'z' in new:
                z_got = new['z']
            if 'gain' in new:
                gain_sum = gain_sum + new['gain']
            if 'hop1' in new:
                hop1[units[t - 2]] = new['hop1']
            if 'hop2' in new:
                hop2[units[t - 3]] = new['hop2']
            ready += [(v, row, at(j, c, 1 - core)) for (j, c, row, _), v in zip(share, new['share'])]
            if 'rest_rec' in new:
                ready.append((new['rest_own'] + new['rest_rec'], 0, rest_tile))
        grad_gain = gain_sum.reshape(hid)
        return loss_mean, grad_rows.reshape(hidden.shape), out, grad_gain

    return jax.shard_map(local_step, mesh=mesh, in_specs=(P('dp', None, None), P('dp', None), P('dp', None), P(None), P(None, 'tp')), out_specs=(P(), P('dp', None, None), P(None, 'tp'), P(None)), check_vma=False)
```
